256 devices in a mesh: replica: 2 (over core), fsdp: 128 (over z, x, y).
Axes of the slice: x: 4, y: 4, z: 8, core: 2. Of those that a mesh axis runs over, the one named last changes fastest.
Arguments:
- activations: bfloat16 [131072, 4096], P(('replica', 'fsdp')), may hold values from -24 to 24
- queries: bfloat16 [131072, 2048], P(('replica', 'fsdp')), may hold values from -60 to 60
- out_grad: bfloat16 [131072, 2048], P(('replica', 'fsdp')), may hold values from -6 to 6
- lengths: int32 [512], P(('replica', 'fsdp')), may hold values from 32 to 256
- norm_gain: float32 [4096], replicated, may hold values from 0.5 to 7
- key_master: float32 [4096, 512], P('fsdp'), may hold values from -0.09375 to 0.09375
- value_master: float32 [4096, 512], P('fsdp'), may hold values from -0.09375 to 0.09375
Outputs:
- key_direction: float32 [4096, 512], P('fsdp')
- value_direction: float32 [4096, 512], P('fsdp')
The draws below stay inside these ranges and needn't reach their ends.
All inputs are finite; a program needn't handle non-finite values.
Results may differ from the reference program's by a relative error of at most 0.009.
The reference program's roundings to bfloat16 on the way (of `normed`, `attended`, `value_grad`, `score_grad` and `key_grad`) count: a program that leaves them out, or rounds other values in their place, can miss the bound.
Values may be sent and summed in bfloat16 or wider, within the bound.
No kernel may reach another device: no remote copies, remote signals or barrier semaphores. Data moves between devices by JAX's collectives and lax.ppermute only.
A program may use at most 128 MiB of HBM per device.

```python
import jax
import jax.numpy as jnp
from jax import lax

D = 4096
HD = 128
KVH = 4
GROUP = 4
LEN = 256
KVW = 512
QW = 2048
SEQS = 512
TOKENS = 131072
N_FSDP = 128


def draw_queries(key, part):
    baseline = jax.random.truncated_normal(key, -4.0, 4.0, (TOKENS, QW), jnp.float32)
    return baseline.astype(jnp.bfloat16)


def draw_norm_gain(key, part):
    row_index = jnp.arange(D, dtype=jnp.int32)
    block_rows = D // N_FSDP
    whole_frac = row_index.astype(jnp.float32) / D
    block_frac = (row_index % block_rows).astype(jnp.float32) / block_rows
    rough = jax.random.uniform(jax.random.fold_in(key, 11), (D,), jnp.float32, 0.85, 1.15)
    ramp = jnp.exp(jnp.log(3.0) * (0.6 * whole_frac + 0.6 * block_frac))
    return (ramp * rough).astype(jnp.float32)


def with_ends(result, key, least, high):
    longest = result.shape.index(max(result.shape))
    spots = []
    for shift in (0, 1):
        where = [jax.random.randint(jax.random.fold_in(key, axis), (), 0, length) for axis, length in enumerate(result.shape)]
        where[longest] = (where[longest] + shift) % result.shape[longest]
        spots.append(tuple(where))
    return result.at[spots[0]].set(least).at[spots[1]].set(high)


def with_spikes(result, key, source, target, shards_of, factor):
    def block_of(dim):
        return (jnp.arange(result.shape[dim]) // (result.shape[dim] // shards_of)).reshape((-1,) + (1,) * (result.ndim - 1 - dim))

    one_side = jax.random.permutation(key, shards_of)[block_of(target)]
    other_side = (block_of(target) + shards_of // 2) % shards_of
    return jnp.where((block_of(source) == one_side) | (block_of(source) == other_side), factor * result, result)


def level_of(key, dims, split, least, largest):
    level = 1.0
    for position, blocks in split:
        steps = jax.random.uniform(jax.random.fold_in(jax.random.fold_in(key, 6), position), (blocks,), jnp.float32, least / len(split), largest / len(split))
        level = level * jnp.repeat(jnp.exp(steps), dims[position] // blocks).reshape((-1,) + (1,) * (len(dims) - 1 - position))
    return level


def bell_draw(stream_key, shape, spread, limit, cuts=(), kind=jnp.bfloat16):
    drawn = jax.random.normal(stream_key, shape, jnp.float32) * spread
    if len(cuts) > 0:
        drawn = level_of(stream_key, shape, cuts, -0.22, 0.18) * drawn
    return jnp.clip(drawn, min=-limit, max=limit).astype(kind)


def heavy_noise(rng, shape, deviation, most, cuts, heavy, held_as=jnp.bfloat16):
    result = deviation * jax.random.normal(rng, shape, jnp.float32)
    if cuts:
        result = result * level_of(rng, shape, cuts, -0.22, 0.18)
    return jnp.clip(with_spikes(result, jax.random.fold_in(rng, 3), *heavy), -most, most).astype(held_as)


def setup_inputs(seed: int = 0) -> dict:
    key_of = jax.random.split(jax.random.key(seed), 8)
    return {
        "activations": heavy_noise(key_of[0], (TOKENS, D), 1.0, 24.0, ((0, 256),), (0, 1, 256, 6.0)),
        "queries": draw_queries(jax.random.fold_in(key_of[7], 71), 0),
        "out_grad": bell_draw(key_of[2], (TOKENS, QW), 1.0, 6.0, ((0, 256),)),
        "lengths": with_ends(jax.random.randint(key_of[3], (SEQS,), LEN // 8, LEN + 1), jax.random.fold_in(key_of[3], 1), LEN // 8, LEN).astype(jnp.int32),
        "norm_gain": draw_norm_gain(jax.random.fold_in(key_of[7], 71), 0),
        "key_master": bell_draw(key_of[5], (D, KVW), D ** -0.5, 0.09375, ((0, 128),), jnp.float32),
        "value_master": bell_draw(key_of[6], (D, KVW), D ** -0.5, 0.09375, ((0, 128),), jnp.float32),
    }


def attend(query_seq, key_seq, value_seq, grad_seq, length):
    scale_factor = 1.0 / HD ** 0.5
    positions = jnp.arange(LEN, dtype=jnp.int32)
    allowed = (positions[None, :] <= positions[:, None]) & (positions[None, :] < length)
    query_float = query_seq.astype(jnp.float32).reshape(LEN, KVH, GROUP, HD)
    key_float = key_seq.astype(jnp.float32).reshape(LEN, KVH, HD)
    value_float = value_seq.astype(jnp.float32).reshape(LEN, KVH, HD)
    scores = jnp.einsum('qhgd,khd->hgqk', query_float, key_float) * scale_factor
    scores = jnp.where(allowed[None, None], scores, jnp.float32(-1e+30))
    row_peak = lax.optimization_barrier(jnp.max(scores, axis=-1, keepdims=True))
    exponent = jnp.exp(scores - row_peak)
    probs = exponent / lax.optimization_barrier(jnp.sum(exponent, axis=-1, keepdims=True))
    probs_low = lax.optimization_barrier(probs.astype(jnp.bfloat16))
    probs_back = probs_low.astype(jnp.float32)
    attended = jnp.einsum('hgqk,khd->qhgd', probs_back, value_float).astype(jnp.bfloat16)
    attended = lax.optimization_barrier(attended).astype(jnp.float32)
    live_rows = (positions < length).astype(jnp.float32)
    grad_float = grad_seq.astype(jnp.float32).reshape(LEN, KVH, GROUP, HD) * live_rows[:, None, None, None]
    row_delta = jnp.transpose(lax.optimization_barrier(jnp.sum(grad_float * attended, axis=-1)), (1, 2, 0))[..., None]
    value_grad = jnp.einsum('hgqk,qhgd->khd', probs_back, grad_float).astype(jnp.bfloat16)
    prob_grad = jnp.einsum('qhgd,khd->hgqk', grad_float, value_float)
    score_grad = lax.optimization_barrier((probs * (prob_grad - row_delta)).astype(jnp.bfloat16))
    key_grad = (jnp.einsum('hgqk,qhgd->khd', score_grad.astype(jnp.float32), query_float) * scale_factor).astype(jnp.bfloat16)
    return (key_grad.reshape(LEN, KVH * HD), value_grad.reshape(LEN, KVH * HD))

def reference(activations, queries, out_grad, lengths, norm_gain, key_master, value_master):
    act_float = activations.astype(jnp.float32)
    inverse = lax.rsqrt(lax.optimization_barrier(jnp.mean(act_float * act_float, axis=-1, keepdims=True)) + 1e-05)
    normed = (act_float * inverse * norm_gain[None, :]).astype(jnp.bfloat16)
    key_proj = jnp.dot(normed, key_master.astype(jnp.bfloat16), preferred_element_type=jnp.float32).astype(jnp.bfloat16)
    value_proj = jnp.dot(normed, value_master.astype(jnp.bfloat16), preferred_element_type=jnp.float32).astype(jnp.bfloat16)
    width = KVH * HD
    qwidth = KVH * GROUP * HD

    def one_seq(packed):
        return attend(packed[0], packed[1], packed[2], packed[3], packed[4])
    key_grad, value_grad = lax.map(one_seq, (queries.reshape(SEQS, LEN, qwidth), key_proj.reshape(SEQS, LEN, width), value_proj.reshape(SEQS, LEN, width), out_grad.reshape(SEQS, LEN, qwidth), lengths))
    key_grad = key_grad.reshape(TOKENS, width)
    value_grad = value_grad.reshape(TOKENS, width)
    key_weight_grad = jnp.dot(normed.T, key_grad, preferred_element_type=jnp.float32)
    value_weight_grad = jnp.dot(normed.T, value_grad, preferred_element_type=jnp.float32)
    total_sq = jnp.sum(key_weight_grad * key_weight_grad) + jnp.sum(value_weight_grad * value_weight_grad)
    unit_scale = jnp.sqrt(jnp.float32(2 * D * width)) / jnp.sqrt(total_sq + 1e-06)
    return (unit_scale * key_weight_grad, unit_scale * value_weight_grad)
```

```python
import functools

import jax
import jax.numpy as jnp
from jax import lax
from jax.experimental import pallas as pl
from jax.experimental.pallas import tpu as pltpu
from jax.sharding import Mesh
from jax.sharding import PartitionSpec as P

D = 4096
HD = 128
GROUP = 4
LEN = 256
EPS = 1e-5
ZN, XN, YN = 8, 4, 4
FSDP = ("z", "x", "y")
ALL = ("r", "z", "x", "y")
BF = jnp.bfloat16
F32 = jnp.float32


def plane_pairs(phase, step):
    pairs = []
    for r in range(2):
        along_x = (r == 1) == (phase == 1)
        for z in range(ZN):
            for x in range(XN):
                for y in range(YN):
                    to = ((x + step) % XN, y) if along_x else (x, (y + step) % YN)
                    here = ((r * ZN + z) * XN + x) * YN + y
                    pairs.append((here, ((r * ZN + z) * XN + to[0]) * YN + to[1]))
    return pairs


def shift(a, phase, step):
    return lax.ppermute(a, ALL, plane_pairs(phase, step))


def to_partner(a):
    return lax.ppermute(a, "r", [(0, 1), (1, 0)])


def exchange(blocks, axes):
    return lax.all_to_all(blocks, axes, split_axis=0, concat_axis=0, tiled=True)


def to_all(a, axes, count):
    return exchange(jnp.broadcast_to(a[None], (count, *a.shape)), axes)


def prep_kernel(where, lengths, act, queries, grad, gain, send, kept):
    i = pl.program_id(0)
    rows = act.shape[0]
    a = act[...].astype(F32)
    inverse = lax.rsqrt(jnp.mean(a * a, axis=-1, keepdims=True) + EPS)
    send[:, :D] = (a * inverse * gain[...]).astype(BF)
    seq = i * rows // LEN
    first = i * rows - seq * LEN
    position = first + lax.broadcasted_iota(jnp.int32, (rows, 1), 0)
    live = position < lengths[seq]
    half = queries.shape[1] // 2
    mine = pl.multiple_of(where[0] * half, half)
    other = pl.multiple_of((1 - where[0]) * half, half)
    send[:, D : D + half] = queries[:, pl.ds(other, half)]
    zero = jnp.zeros((rows, half), BF)
    send[:, D + half :] = jnp.where(live, grad[:, pl.ds(other, half)], zero)
    kept[...] = jnp.where(live, grad[:, pl.ds(mine, half)], zero)


def prepare(where, lengths, act, queries, grad, gain):
    tokens, width = act.shape[0], queries.shape[1]
    rows = 128
    return pl.pallas_call(
        prep_kernel,
        grid_spec=pltpu.PrefetchScalarGridSpec(
            num_scalar_prefetch=2,
            grid=(tokens // rows,),
            in_specs=[
                pl.BlockSpec((rows, D), lambda i, *_: (i, 0)),
                pl.BlockSpec((rows, width), lambda i, *_: (i, 0)),
                pl.BlockSpec((rows, width), lambda i, *_: (i, 0)),
                pl.BlockSpec((1, D), lambda i, *_: (0, 0)),
            ],
            out_specs=[
                pl.BlockSpec((rows, D + width), lambda i, *_: (i, 0)),
                pl.BlockSpec((rows, width // 2), lambda i, *_: (i, 0)),
            ],
        ),
        out_shape=[
            jax.ShapeDtypeStruct((tokens, D + width), BF),
            jax.ShapeDtypeStruct((tokens, width // 2), BF),
        ],
        name="prep",
    )(where, lengths, act, queries, grad, gain.reshape(1, D))


NT = (((1,), (1,)), ((), ()))
CHUNK = 128


def head_kernel(head, where, w0, w1, w2, w3, sent, came, queries, kept,
                g0, g1, g2, g3, normed, q, go, w, kv, dkvt, block, sems):
    half = queries.shape[0]
    wide = GROUP * HD
    base = pl.multiple_of(where[0] * (queries.shape[1] // 2) + head * wide, wide)
    qcol = D + head * wide
    gcol = D + queries.shape[1] // 2 + head * wide
    copies = []
    for i in range(2 * half // CHUNK):
        at = i * CHUNK % half
        source = sent if i * CHUNK < half else came
        copies.append(pltpu.make_async_copy(
            source.at[pl.ds(at, CHUNK), pl.ds(0, D)], normed.at[pl.ds(i * CHUNK, CHUNK)], sems.at[i]))
    n = len(copies)
    small = [
        pltpu.make_async_copy(queries.at[:, pl.ds(base, wide)], q.at[pl.ds(0, half)], sems.at[n]),
        pltpu.make_async_copy(came.at[:, pl.ds(qcol, wide)], q.at[pl.ds(half, half)], sems.at[n + 1]),
        pltpu.make_async_copy(kept.at[:, pl.ds(head * wide, wide)], go.at[pl.ds(0, half)], sems.at[n + 2]),
        pltpu.make_async_copy(came.at[:, pl.ds(gcol, wide)], go.at[pl.ds(half, half)], sems.at[n + 3]),
    ]
    for c in copies + small:
        c.start()
    p1, p2, s1, s2 = where[1], where[2], where[3], where[4]

    def chunk_at(o1, o2):
        return pl.multiple_of((lax.rem(p1 + o1, 4) * s1 + lax.rem(p2 + o2, 4) * s2) * 32, 32)

    for o2, source in enumerate((w0, w1, w2, w3)):
        for o1 in range(4):
            at = chunk_at(o1, o2)
            for z in range(ZN):
                w[pl.ds(z * 512 + at, 32)] = source[o1, z]
    for i, c in enumerate(copies):
        c.wait()
        rows = pl.ds(i * CHUNK, CHUNK)
        kv[rows] = jnp.dot(normed[rows], w[...], preferred_element_type=F32).astype(BF)
    for c in small:
        c.wait()
    scale = 1.0 / HD**0.5
    allowed = lax.broadcasted_iota(jnp.int32, (LEN, LEN), 0) <= lax.broadcasted_iota(jnp.int32, (LEN, LEN), 1)

    def one_seq(s, _):
        rows = pl.ds(pl.multiple_of(s * LEN, LEN), LEN)
        key, value = kv[rows, :HD], kv[rows, HD:]
        value_t = value.T
        dk = jnp.zeros((LEN, HD), F32)
        dv = jnp.zeros((LEN, HD), F32)
        for g in range(GROUP):
            cols = slice(g * HD, (g + 1) * HD)
            qg, gg = q[rows, cols], go[rows, cols]
            score = lax.dot_general(key, qg, NT, preferred_element_type=F32) * scale
            score = jnp.where(allowed, score, -1e30)
            e = jnp.exp(score - jnp.max(score, axis=0, keepdims=True))
            p = e * (1.0 / jnp.sum(e, axis=0, keepdims=True))
            pb = p.astype(BF)
            out_t = jnp.dot(value_t, pb, preferred_element_type=F32).astype(BF).astype(F32)
            delta = jnp.sum(gg.T.astype(F32) * out_t, axis=0, keepdims=True)
            dp = lax.dot_general(value, gg, NT, preferred_element_type=F32)
            ds = (p * (dp - delta)).astype(BF)
            dv += jnp.dot(pb, gg, preferred_element_type=F32)
            dk += jnp.dot(ds, qg, preferred_element_type=F32)
        both = jnp.concatenate([(dk * scale).astype(BF), dv.astype(BF)], axis=1)
        dkvt[:, rows] = both.T
        return 0

    lax.fori_loop(0, 2 * half // LEN, one_seq, 0)
    for z in range(ZN):
        part = jnp.dot(dkvt[...], normed[:, z * 512 : (z + 1) * 512], preferred_element_type=F32)
        block[...] = part.astype(BF).T
        for o2, target in enumerate((g0, g1, g2, g3)):
            for o1 in range(4):
                target[o1, z] = block[pl.ds(chunk_at(o1, o2), 32)]


def one_head(head, where, pieces, sent, came, queries, kept):
    tokens = 2 * queries.shape[0]
    vmem = pl.BlockSpec(memory_space=pltpu.VMEM)
    hbm = pl.BlockSpec(memory_space=pl.ANY)
    cols = 2 * HD
    wide = GROUP * HD
    return pl.pallas_call(
        functools.partial(head_kernel, head),
        in_specs=[pl.BlockSpec(memory_space=pltpu.SMEM)] + [vmem] * 4 + [hbm] * 4,
        out_specs=[vmem] * 4,
        out_shape=[jax.ShapeDtypeStruct((4, ZN, 32, cols), BF)] * 4,
        scratch_shapes=[
            pltpu.VMEM((tokens, D), BF),
            pltpu.VMEM((tokens, wide), BF),
            pltpu.VMEM((tokens, wide), BF),
            pltpu.VMEM((D, cols), BF),
            pltpu.VMEM((tokens, cols), BF),
            pltpu.VMEM((cols, tokens), BF),
            pltpu.VMEM((512, cols), BF),
            pltpu.SemaphoreType.DMA((tokens // CHUNK + 4,)),
        ],
        compiler_params=pltpu.CompilerParams(vmem_limit_bytes=40 * 2**20),
        cost_estimate=pl.CostEstimate(flops=8_000_000_000, transcendentals=1_000_000, bytes_accessed=16_000_000),
        name=f"head{head}",
    )(where, *pieces, sent, came, queries, kept)


def local(activations, queries, out_grad, lengths, norm_gain, key_master, value_master):
    r, x, y = lax.axis_index("r"), lax.axis_index("x"), lax.axis_index("y")
    first = r == 0
    where = jnp.stack([
        r,
        jnp.where(first, y, x), jnp.where(first, x, y),
        jnp.where(first, 1, 4), jnp.where(first, 4, 1),
    ]).astype(jnp.int32)

    def mine(a):
        a = lax.dynamic_slice_in_dim(a, r * 2 * HD, 2 * HD, axis=1).astype(BF)
        return a.reshape(32, 2, HD).transpose(1, 0, 2)

    own = jnp.concatenate([mine(key_master), mine(value_master)], axis=2)
    sent, kept = prepare(where, lengths, activations, queries, out_grad, norm_gain)
    came = to_partner(sent)
    level = to_all(own, "z", ZN)
    level = [level] + [shift(level, 1, -o) for o in (1, 2, 3)]
    outs = []
    pieces = []
    for head in range(2):
        block = jnp.stack([a[:, head] for a in level])
        pieces.append([block] + [shift(block, 2, -o) for o in (1, 2, 3)])
    for head in range(2):
        g = one_head(head, where, pieces[head], sent, came, queries, kept)
        got = [g[0]] + [shift(g[o], 2, o) for o in (1, 2, 3)]
        outs.append(sum(a.astype(F32) for a in got).astype(BF))
    both = jnp.stack(outs, axis=1)
    got = [both[0]] + [shift(both[o], 1, o) for o in (1, 2, 3)]
    part = sum(a.astype(F32) for a in got).astype(BF)
    full = exchange(part.transpose(1, 0, 2, 3), "z").astype(F32).sum(axis=0)
    square = jnp.full((1, 128), jnp.sum(full * full) / 128, F32)
    theirs = to_partner(full)
    total = jnp.sum(to_all(square, FSDP, 128), axis=(0, 1))
    total = total + to_partner(total)
    scale = jnp.sqrt(jnp.float32(2 * D * 512)) / jnp.sqrt(jnp.sum(total) + 1e-6)
    low = jnp.where(first, full, theirs)
    high = jnp.where(first, theirs, full)
    whole = jnp.concatenate([low, high]) * scale
    key = whole[:, :, :HD].transpose(1, 0, 2).reshape(32, 4 * HD)
    value = whole[:, :, HD:].transpose(1, 0, 2).reshape(32, 4 * HD)
    return key, value


def solution(mesh):
    split = Mesh(mesh.devices.reshape(2, ZN, XN, YN), ALL)
    in_specs = (P(ALL, None), P(ALL, None), P(ALL, None), P(ALL), P(), P(FSDP, None), P(FSDP, None))
    out_specs = (P(FSDP, None), P(FSDP, None))
    return jax.shard_map(local, mesh=split, in_specs=in_specs, out_specs=out_specs, check_vma=False)
```

```python
import functools

import jax
import jax.numpy as jnp
from jax import lax
from jax.experimental import pallas as pl
from jax.experimental.pallas import tpu as pltpu
from jax.sharding import Mesh
from jax.sharding import PartitionSpec as P


D = 4096
HD = 128
GROUP = 4
LEN = 256
EPS = 1e-5
ZN, XN, YN = 8, 4, 4
FSDP = ("z", "x", "y")
ALL = ("r", "z", "x", "y")
BF = jnp.bfloat16
F32 = jnp.float32


def plane_pairs(phase, step):
    pairs = []
    for r in range(2):
        along_x = (r == 1) == (phase == 1)
        for z in range(ZN):
            for x in range(XN):
                for y in range(YN):
                    to = ((x + step) % XN, y) if along_x else (x, (y + step) % YN)
                    here = ((r * ZN + z) * XN + x) * YN + y
                    pairs.append((here, ((r * ZN + z) * XN + to[0]) * YN + to[1]))
    return pairs


def shift(a, phase, step):
    return lax.ppermute(a, ALL, plane_pairs(phase, step))


def level_pair(a):
    return lax.ppermute(a, "z", [(i, i ^ 1) for i in range(ZN)])


def level_shift(a, k):
    return lax.ppermute(a, "z", [(i, (i + 2 * k) % ZN) for i in range(ZN)])


def to_partner(a):
    return lax.ppermute(a, "r", [(0, 1), (1, 0)])


def exchange(blocks, axes):
    return lax.all_to_all(blocks, axes, split_axis=0, concat_axis=0, tiled=True)


def in_hbm(a):
    return pltpu.with_memory_space_constraint(a, pltpu.HBM)


def cast_kernel(key, value, own, key_in, value_in, sems):
    cols = pl.ds(pl.multiple_of(lax.axis_index("r") * 2 * HD, 2 * HD), 2 * HD)
    loads = [
        pltpu.make_async_copy(key.at[:, cols], key_in, sems.at[0]),
        pltpu.make_async_copy(value.at[:, cols], value_in, sems.at[1]),
    ]
    for c in loads:
        c.start()
    for c in loads:
        c.wait()
    for h in range(2):
        own[h, :, :HD] = key_in[:, h * HD : (h + 1) * HD].astype(BF)
        own[h, :, HD:] = value_in[:, h * HD : (h + 1) * HD].astype(BF)


def cast(key, value):
    rows = key.shape[0]
    hbm = pl.BlockSpec(memory_space=pltpu.HBM)
    return pl.pallas_call(
        cast_kernel,
        in_specs=[hbm, hbm],
        out_specs=pl.BlockSpec(memory_space=pltpu.VMEM),
        out_shape=pltpu.VMEM((2, rows, 2 * HD), BF),
        scratch_shapes=[
            pltpu.VMEM((rows, 2 * HD), F32),
            pltpu.VMEM((rows, 2 * HD), F32),
            pltpu.SemaphoreType.DMA((2,)),
        ],
        compiler_params=pltpu.CompilerParams(vmem_limit_bytes=4 * 2**20),
        name="cast",
    )(in_hbm(key), in_hbm(value))


ROWS = 64


def prep_kernel(where, act, queries, grad, gain, send, kept, rows_in, grad_in, gain_in, sems):
    tokens, half = act.shape[0], queries.shape[1] // 2
    steps = tokens // ROWS
    mine = pl.multiple_of(where[0] * half, half)
    other = pl.multiple_of((1 - where[0]) * half, half)
    swap = pltpu.make_async_copy(queries.at[:, pl.ds(other, half)], send.at[:, pl.ds(D, half)], sems.at[2 * steps])
    loads = []
    for i in range(steps):
        at = pl.ds(i * ROWS, ROWS)
        loads.append((
            pltpu.make_async_copy(act.at[at], rows_in.at[at], sems.at[i]),
            pltpu.make_async_copy(grad.at[at], grad_in.at[at], sems.at[steps + i]),
        ))
    for pair in loads:
        pair[0].start()
        pair[1].start()
    swap.start()
    gain_load = pltpu.make_async_copy(gain, gain_in, sems.at[2 * steps + 1])
    gain_load.start()
    gain_load.wait()
    zero = jnp.zeros((ROWS, half), BF)
    for i in range(steps):
        at = slice(i * ROWS, (i + 1) * ROWS)
        loads[i][0].wait()
        loads[i][1].wait()
        a = rows_in[at].astype(F32)
        inverse = lax.rsqrt(jnp.mean(a * a, axis=-1, keepdims=True) + EPS)
        send[at, :D] = (a * inverse * gain_in[...]).astype(BF)
        seq = i * ROWS // LEN
        live = i * ROWS - seq * LEN + lax.broadcasted_iota(jnp.int32, (ROWS, 1), 0) < where[6 + seq]
        send[at, D + half :] = jnp.where(live, grad_in[at, pl.ds(other, half)], zero)
        kept[at] = jnp.where(live, grad_in[at, pl.ds(mine, half)], zero)
    swap.wait()


def prepare(where, act, queries, grad, gain):
    tokens, width = act.shape[0], queries.shape[1]
    vmem = pl.BlockSpec(memory_space=pltpu.VMEM)
    smem = pl.BlockSpec(memory_space=pltpu.SMEM)
    hbm = pl.BlockSpec(memory_space=pltpu.HBM)
    return pl.pallas_call(
        prep_kernel,
        in_specs=[smem, hbm, hbm, hbm, hbm],
        out_specs=[vmem, vmem],
        out_shape=[
            pltpu.VMEM((tokens, D + width), BF),
            pltpu.VMEM((tokens, width // 2), BF),
        ],
        scratch_shapes=[
            pltpu.VMEM((tokens, D), BF),
            pltpu.VMEM((tokens, width), BF),
            pltpu.VMEM((1, D), F32),
            pltpu.SemaphoreType.DMA((2 * (tokens // ROWS) + 2,)),
        ],
        compiler_params=pltpu.CompilerParams(vmem_limit_bytes=24 * 2**20),
        cost_estimate=pl.CostEstimate(flops=1_000_000_000, transcendentals=512, bytes_accessed=16_000_000),
        name="prep",
    )(where, *(in_hbm(a) for a in (act, queries, grad, gain.reshape(1, D))))


def merge_kernel(keep, got, far, crossed, full, theirs, square):
    full[...] = keep[...] + got[...].astype(F32)
    theirs[...] = far[...] + crossed[...].astype(F32)
    total = jnp.sum(full[...] * full[...]) + jnp.sum(theirs[...] * theirs[...])
    square[...] = jnp.full(square.shape, total, F32)


def merge(keep, got, far, crossed):
    vmem = pl.BlockSpec(memory_space=pltpu.VMEM)
    like = jax.ShapeDtypeStruct(keep.shape, F32)
    return pl.pallas_call(
        merge_kernel,
        in_specs=[vmem] * 4,
        out_specs=[vmem] * 3,
        out_shape=[like, like, jax.ShapeDtypeStruct((128, 1, 128), F32)],
        compiler_params=pltpu.CompilerParams(vmem_limit_bytes=4 * 2**20),
        name="merge",
    )(keep, got, far, crossed)


def finish_kernel(where, squares, full, theirs, key, value):
    total = jnp.sum(squares[...]) / 128
    scale = jnp.sqrt(jnp.float32(2 * D * 512)) / jnp.sqrt(total + 1e-6)
    for r in range(2):
        for h in range(2):
            both = jnp.where(where[0] == r, full[h], theirs[h]) * scale
            cols = slice((2 * r + h) * HD, (2 * r + h + 1) * HD)
            key[:, cols] = both[:, :HD]
            value[:, cols] = both[:, HD:]


def finish(where, squares, full, theirs):
    vmem = pl.BlockSpec(memory_space=pltpu.VMEM)
    like = jax.ShapeDtypeStruct((32, 4 * HD), F32)
    return pl.pallas_call(
        finish_kernel,
        in_specs=[pl.BlockSpec(memory_space=pltpu.SMEM)] + [vmem] * 3,
        out_specs=[vmem] * 2,
        out_shape=[like, like],
        compiler_params=pltpu.CompilerParams(vmem_limit_bytes=4 * 2**20),
        name="finish",
    )(where, squares, full, theirs)


NT = (((1,), (1,)), ((), ()))


def head_kernel(head, where, w0, w1, w2, w3, sent, came, queries, kept, g0, g1, g2, g3, w, kv, dkvt, block):
    half = queries.shape[0]
    wide = GROUP * HD
    base = pl.multiple_of(where[0] * (queries.shape[1] // 2) + head * wide, wide)
    qcol = D + head * wide
    gcol = D + queries.shape[1] // 2 + head * wide
    p1, p2, s1, s2, z0 = where[1], where[2], where[3], where[4], where[5]

    def chunk_at(o1, o2):
        return pl.multiple_of((lax.rem(p1 + o1, 4) * s1 + lax.rem(p2 + o2, 4) * s2) * 32, 32)

    def level_at(i):
        even = lax.rem(z0 + i - i % 2, ZN)
        at = even if i % 2 == 0 else even + 1 - 2 * lax.rem(even, 2)
        return pl.multiple_of(at * 512, 512)

    for o2, source in enumerate((w0, w1, w2, w3)):
        for o1 in range(4):
            at = chunk_at(o1, o2)
            for z in range(ZN):
                w[pl.ds(level_at(z) + at, 32)] = source[o1, z]

    def project(s):
        source = sent if s * LEN < half else came
        at = s * LEN % half
        kv[s * LEN : (s + 1) * LEN] = jnp.dot(source[at : at + LEN, :D], w[...], preferred_element_type=F32).astype(BF)

    project(0)
    scale = 1.0 / HD**0.5
    top = HD
    below = lax.broadcasted_iota(jnp.int32, (top, top), 0) <= lax.broadcasted_iota(jnp.int32, (top, top), 1)

    def stacked(ref, rows, col):
        return jnp.concatenate([ref[rows, pl.ds(col + g * HD, HD)] for g in range(GROUP)], axis=0)

    def soft(parts):
        peak = functools.reduce(jnp.maximum, [jnp.max(a, axis=0, keepdims=True) for a in parts])
        parts = [jnp.exp(a - peak) for a in parts]
        inverse = 1.0 / functools.reduce(jnp.add, [jnp.sum(a, axis=0, keepdims=True) for a in parts])
        return [a * inverse for a in parts]

    def strip(key, value, value_t, qs, gs):
        keys = key.shape[0]
        score = lax.dot_general(key, qs, NT, preferred_element_type=F32)
        dp = lax.dot_general(value, gs, NT, preferred_element_type=F32)
        ps, pbs = [], []
        for g in range(GROUP):
            cols = slice(g * top, (g + 1) * top)
            parts = [score[i : i + top, cols] * scale for i in range(0, keys, top)]
            parts[-1] = jnp.where(below, parts[-1], -1e30)
            p = jnp.concatenate(soft(parts), axis=0)
            ps.append(p)
            pbs.append(p.astype(BF))
        pb = jnp.concatenate(pbs, axis=1)
        out_t = jnp.dot(value_t, pb, preferred_element_type=F32).astype(BF).astype(F32)
        delta = jnp.sum(gs.T.astype(F32) * out_t, axis=0, keepdims=True)
        ds = []
        for g in range(GROUP):
            cols = slice(g * top, (g + 1) * top)
            ds.append((ps[g] * (dp[:, cols] - delta[:, cols])).astype(BF))
        ds = jnp.concatenate(ds, axis=1)
        return jnp.dot(ds, qs, preferred_element_type=F32), jnp.dot(pb, gs, preferred_element_type=F32)

    for s in range(2 * half // LEN):
        rows = slice(s * LEN, (s + 1) * LEN)
        at = s * LEN % half
        qref, qat, gref, gat = (queries, base, kept, head * wide) if s * LEN < half else (came, qcol, came, gcol)
        key, value = kv[rows, :HD], kv[rows, HD:]
        value_t = value.T
        if (s + 1) * LEN < 2 * half:
            project(s + 1)
        early, late = slice(at, at + top), slice(at + top, at + LEN)
        dk0, dv0 = strip(key[:top], value[:top], value_t[:, :top], stacked(qref, early, qat), stacked(gref, early, gat))
        dk1, dv1 = strip(key, value, value_t, stacked(qref, late, qat), stacked(gref, late, gat))
        dk = jnp.concatenate([dk1[:top] + dk0, dk1[top:]], axis=0)
        dv = jnp.concatenate([dv1[:top] + dv0, dv1[top:]], axis=0)
        both = jnp.concatenate([(dk * scale).astype(BF), dv.astype(BF)], axis=1)
        dkvt[:, rows] = both.T

    for z in range(ZN):
        cols = pl.ds(level_at(z), 512)
        part = jnp.dot(dkvt[:, :half], sent[:, cols], preferred_element_type=F32)
        part += jnp.dot(dkvt[:, half:], came[:, cols], preferred_element_type=F32)
        block[...] = part.astype(BF).T
        for o2, target in enumerate((g0, g1, g2, g3)):
            for o1 in range(4):
                target[o1, z] = block[pl.ds(chunk_at(o1, o2), 32)]


def one_head(head, where, pieces, sent, came, queries, kept):
    tokens = 2 * queries.shape[0]
    vmem = pl.BlockSpec(memory_space=pltpu.VMEM)
    cols = 2 * HD
    return pl.pallas_call(
        functools.partial(head_kernel, head),
        in_specs=[pl.BlockSpec(memory_space=pltpu.SMEM)] + [vmem] * 8,
        out_specs=[vmem] * 4,
        out_shape=[jax.ShapeDtypeStruct((4, ZN, 32, cols), BF)] * 4,
        scratch_shapes=[
            pltpu.VMEM((D, cols), BF),
            pltpu.VMEM((tokens, cols), BF),
            pltpu.VMEM((cols, tokens), BF),
            pltpu.VMEM((512, cols), BF),
        ],
        compiler_params=pltpu.CompilerParams(vmem_limit_bytes=30 * 2**20),
        cost_estimate=pl.CostEstimate(flops=8_000_000_000, transcendentals=1_000_000, bytes_accessed=16_000_000),
    )(where, *pieces, sent, came, queries, kept)


def local(activations, queries, out_grad, lengths, norm_gain, key_master, value_master):
    r, z, x, y = (lax.axis_index(a) for a in ALL)
    first = r == 0
    where = jnp.stack([
        r,
        jnp.where(first, y, x), jnp.where(first, x, y),
        jnp.where(first, 1, 4), jnp.where(first, 4, 1),
        z, lengths[0], lengths[1],
    ]).astype(jnp.int32)

    own = cast(key_master, value_master)
    pair = jnp.stack([own, level_pair(own)])
    level = jnp.concatenate([pair] + [level_shift(pair, -k) for k in (1, 2, 3)])
    sent, kept = prepare(where, activations, queries, out_grad, norm_gain)
    came = to_partner(sent)
    gathered = [level]
    for o in (1, 2, 3):
        gathered.append(shift(level, 1, -o))
    pieces = []
    for head in range(2):
        block = jnp.stack([a[:, head] for a in gathered])
        pieces.append([block] + [shift(block, 2, -o) for o in (1, 2, 3)])
    parts = []
    for head in range(2):
        g = one_head(head, where, pieces[head], sent, came, queries, kept)
        got = [g[0]] + [shift(g[o], 2, o) for o in (1, 2, 3)]
        line = sum(a.astype(F32) for a in got).astype(BF)
        got = [line[0]] + [shift(line[o], 1, o) for o in (1, 2, 3)]
        parts.append(sum(a.astype(F32) for a in got).astype(BF))
    part = jnp.stack(parts, axis=1).reshape(4, 2, 2, 32, 256)
    got = [part[0]] + [level_shift(part[k], k) for k in (1, 2, 3)]
    pair = sum(a.astype(F32) for a in got)
    keep, give = pair[0], pair[1].astype(BF)
    crossed = lax.ppermute(give, ("r", "z"), [(i * ZN + j, (1 - i) * ZN + (j ^ 1)) for i in range(2) for j in range(ZN)])
    full, theirs, square = merge(keep, level_pair(give), to_partner(keep), crossed)
    return finish(where, exchange(square, FSDP), full, theirs)


def solution(mesh):
    split = Mesh(mesh.devices.reshape(2, ZN, XN, YN), ALL)
    in_specs = (P(ALL, None), P(ALL, None), P(ALL, None), P(ALL), P(), P(FSDP, None), P(FSDP, None))
    out_specs = (P(FSDP, None), P(FSDP, None))


    return jax.shard_map(local, mesh=split, in_specs=in_specs, out_specs=out_specs, check_vma=False)
```

```python
import functools

import jax
import jax.numpy as jnp
from jax import lax
from jax.experimental import pallas as pl
from jax.experimental.pallas import tpu as pltpu
from jax.sharding import Mesh
from jax.sharding import PartitionSpec as P


D = 4096
HD = 128
GROUP = 4
LEN = 256
EPS = 1e-5
ZN, XN, YN = 8, 4, 4
FSDP = ("z", "x", "y")
ALL = ("r", "z", "x", "y")
BF = jnp.bfloat16
F32 = jnp.float32


def plane_pairs(phase, step):
    pairs = []
    for r in range(2):
        along_x = (r == 1) == (phase == 1)
        for z in range(ZN):
            for x in range(XN):
                for y in range(YN):
                    to = ((x + step) % XN, y) if along_x else (x, (y + step) % YN)
                    here = ((r * ZN + z) * XN + x) * YN + y
                    pairs.append((here, ((r * ZN + z) * XN + to[0]) * YN + to[1]))
    return pairs


def shift(a, phase, step):
    return lax.ppermute(a, ALL, plane_pairs(phase, step))


def to_partner(a):
    return lax.ppermute(a, "r", [(0, 1), (1, 0)])


def exchange(blocks, axes):
    return lax.all_to_all(blocks, axes, split_axis=0, concat_axis=0, tiled=True)


def in_hbm(a):
    return pltpu.with_memory_space_constraint(a, pltpu.HBM)


def cast_kernel(key, value, own, key_in, value_in, sems):
    cols = pl.ds(pl.multiple_of(lax.axis_index("r") * 2 * HD, 2 * HD), 2 * HD)
    loads = [
        pltpu.make_async_copy(key.at[:, cols], key_in, sems.at[0]),
        pltpu.make_async_copy(value.at[:, cols], value_in, sems.at[1]),
    ]
    for c in loads:
        c.start()
    for c in loads:
        c.wait()
    for h in range(2):
        own[h, :, :HD] = key_in[:, h * HD : (h + 1) * HD].astype(BF)
        own[h, :, HD:] = value_in[:, h * HD : (h + 1) * HD].astype(BF)


def cast(key, value):
    rows = key.shape[0]
    hbm = pl.BlockSpec(memory_space=pltpu.HBM)
    return pl.pallas_call(
        cast_kernel,
        in_specs=[hbm, hbm],
        out_specs=pl.BlockSpec(memory_space=pltpu.VMEM),
        out_shape=pltpu.VMEM((2, rows, 2 * HD), BF),
        scratch_shapes=[
            pltpu.VMEM((rows, 2 * HD), F32),
            pltpu.VMEM((rows, 2 * HD), F32),
            pltpu.SemaphoreType.DMA((2,)),
        ],
        compiler_params=pltpu.CompilerParams(vmem_limit_bytes=4 * 2**20),
        name="cast",
    )(in_hbm(key), in_hbm(value))


ROWS = 64


def prep_kernel(where, act, queries, grad, gain, send, kept, rows_in, grad_in, gain_in, sems):
    tokens, half = act.shape[0], queries.shape[1] // 2
    steps = tokens // ROWS
    mine = pl.multiple_of(where[0] * half, half)
    other = pl.multiple_of((1 - where[0]) * half, half)
    swap = pltpu.make_async_copy(queries.at[:, pl.ds(other, half)], send.at[:, pl.ds(D, half)], sems.at[2 * steps])

    def loads(i):
        at = pl.ds(pl.multiple_of(i * ROWS, ROWS), ROWS)
        return (
            pltpu.make_async_copy(act.at[at], rows_in.at[at], sems.at[i]),
            pltpu.make_async_copy(grad.at[at], grad_in.at[at], sems.at[steps + i]),
        )

    for i in range(steps):
        for c in loads(i):
            c.start()
    swap.start()
    gain_load = pltpu.make_async_copy(gain, gain_in, sems.at[2 * steps + 1])
    gain_load.start()
    gain_load.wait()
    zero = jnp.zeros((ROWS, half), BF)

    def step(i, _):
        at = pl.ds(pl.multiple_of(i * ROWS, ROWS), ROWS)
        for c in loads(i):
            c.wait()
        a = rows_in[at].astype(F32)
        inverse = lax.rsqrt(jnp.mean(a * a, axis=-1, keepdims=True) + EPS)
        send[at, :D] = (a * inverse * gain_in[...]).astype(BF)
        seq = i // (LEN // ROWS)
        live = i * ROWS - seq * LEN + lax.broadcasted_iota(jnp.int32, (ROWS, 1), 0) < where[6 + seq]
        send[at, D + half :] = jnp.where(live, grad_in[at, pl.ds(other, half)], zero)
        kept[at] = jnp.where(live, grad_in[at, pl.ds(mine, half)], zero)
        return 0

    lax.fori_loop(0, steps, step, 0)
    swap.wait()


def prepare(where, act, queries, grad, gain):
    tokens, width = act.shape[0], queries.shape[1]
    vmem = pl.BlockSpec(memory_space=pltpu.VMEM)
    smem = pl.BlockSpec(memory_space=pltpu.SMEM)
    hbm = pl.BlockSpec(memory_space=pltpu.HBM)
    return pl.pallas_call(
        prep_kernel,
        in_specs=[smem, hbm, hbm, hbm, hbm],
        out_specs=[vmem, vmem],
        out_shape=[
            pltpu.VMEM((tokens, D + width), BF),
            pltpu.VMEM((tokens, width // 2), BF),
        ],
        scratch_shapes=[
            pltpu.VMEM((tokens, D), BF),
            pltpu.VMEM((tokens, width), BF),
            pltpu.VMEM((1, D), F32),
            pltpu.SemaphoreType.DMA((2 * (tokens // ROWS) + 2,)),
        ],
        compiler_params=pltpu.CompilerParams(vmem_limit_bytes=24 * 2**20),
        cost_estimate=pl.CostEstimate(flops=1_000_000_000, transcendentals=512, bytes_accessed=16_000_000),
        name="prep",
    )(where, *(in_hbm(a) for a in (act, queries, grad, gain.reshape(1, D))))


def sum_kernel(parts, full):
    full[...] = functools.reduce(jnp.add, [parts[i].astype(F32) for i in range(ZN)])


def gather_sum(parts):
    vmem = pl.BlockSpec(memory_space=pltpu.VMEM)
    return pl.pallas_call(
        sum_kernel,
        in_specs=[vmem],
        out_specs=vmem,
        out_shape=pltpu.VMEM(parts.shape[1:], F32),
        compiler_params=pltpu.CompilerParams(vmem_limit_bytes=4 * 2**20),
        name="gather_sum",
    )(parts)


def square_kernel(full, theirs, square):
    total = jnp.sum(full[...] * full[...]) + jnp.sum(theirs[...] * theirs[...])
    square[...] = jnp.full(square.shape, total, F32)


def squares(full, theirs):
    vmem = pl.BlockSpec(memory_space=pltpu.VMEM)
    return pl.pallas_call(
        square_kernel,
        in_specs=[vmem] * 2,
        out_specs=vmem,
        out_shape=pltpu.VMEM((128, 1, 128), F32),
        compiler_params=pltpu.CompilerParams(vmem_limit_bytes=4 * 2**20),
        name="squares",
    )(full, theirs)


def finish_kernel(where, squares, full, theirs, key, value):
    total = jnp.sum(squares[...]) / 128
    scale = jnp.sqrt(jnp.float32(2 * D * 512)) / jnp.sqrt(total + 1e-6)
    for r in range(2):
        for h in range(2):
            both = jnp.where(where[0] == r, full[h], theirs[h]) * scale
            cols = slice((2 * r + h) * HD, (2 * r + h + 1) * HD)
            key[:, cols] = both[:, :HD]
            value[:, cols] = both[:, HD:]


def finish(where, squares, full, theirs):
    vmem = pl.BlockSpec(memory_space=pltpu.VMEM)
    like = jax.ShapeDtypeStruct((32, 4 * HD), F32)
    return pl.pallas_call(
        finish_kernel,
        in_specs=[pl.BlockSpec(memory_space=pltpu.SMEM)] + [vmem] * 3,
        out_specs=[vmem] * 2,
        out_shape=[like, like],
        compiler_params=pltpu.CompilerParams(vmem_limit_bytes=4 * 2**20),
        name="finish",
    )(where, squares, full, theirs)


NT = (((1,), (1,)), ((), ()))


def head_kernel(which, where, w0, w1, w2, w3, sent, came, queries, kept, g0, g1, g2, g3, w, kv, dkvt, block):
    half = queries.shape[0]
    wide = GROUP * HD
    own = pl.multiple_of(which[0] * wide, wide)
    base = pl.multiple_of(where[0] * (queries.shape[1] // 2) + own, wide)
    qcol = D + own
    gcol = D + queries.shape[1] // 2 + own
    p1, p2, s1, s2 = where[1], where[2], where[3], where[4]

    def chunk_at(o1, o2):
        return pl.multiple_of((lax.rem(p1 + o1, 4) * s1 + lax.rem(p2 + o2, 4) * s2) * 32, 32)

    def level_at(i):
        return i * 512

    for o2, source in enumerate((w0, w1, w2, w3)):
        for o1 in range(4):
            at = chunk_at(o1, o2)
            for z in range(ZN):
                w[pl.ds(level_at(z) + at, 32)] = source[o1, z]

    def project(s):
        source = sent if s * LEN < half else came
        at = s * LEN % half
        kv[s * LEN : (s + 1) * LEN] = jnp.dot(source[at : at + LEN, :D], w[...], preferred_element_type=F32).astype(BF)

    project(0)
    scale = 1.0 / HD**0.5
    top = HD
    below = lax.broadcasted_iota(jnp.int32, (top, top), 0) <= lax.broadcasted_iota(jnp.int32, (top, top), 1)

    def stacked(ref, rows, col):
        return jnp.concatenate([ref[rows, pl.ds(col + g * HD, HD)] for g in range(GROUP)], axis=0)

    def soft(parts):
        peak = functools.reduce(jnp.maximum, [jnp.max(a, axis=0, keepdims=True) for a in parts])
        parts = [jnp.exp(a - peak) for a in parts]
        inverse = 1.0 / functools.reduce(jnp.add, [jnp.sum(a, axis=0, keepdims=True) for a in parts])
        return [a * inverse for a in parts]

    def strip(key, value, value_t, qs, gs):
        keys = key.shape[0]
        score = lax.dot_general(key, qs, NT, preferred_element_type=F32)
        dp = lax.dot_general(value, gs, NT, preferred_element_type=F32)
        ps, pbs = [], []
        for g in range(GROUP):
            cols = slice(g * top, (g + 1) * top)
            parts = [score[i : i + top, cols] * scale for i in range(0, keys, top)]
            parts[-1] = jnp.where(below, parts[-1], -1e30)
            p = jnp.concatenate(soft(parts), axis=0)
            ps.append(p)
            pbs.append(p.astype(BF))
        pb = jnp.concatenate(pbs, axis=1)
        out_t = jnp.dot(value_t, pb, preferred_element_type=F32).astype(BF).astype(F32)
        delta = jnp.sum(gs.T.astype(F32) * out_t, axis=0, keepdims=True)
        ds = []
        for g in range(GROUP):
            cols = slice(g * top, (g + 1) * top)
            ds.append((ps[g] * (dp[:, cols] - delta[:, cols])).astype(BF))
        ds = jnp.concatenate(ds, axis=1)
        return jnp.dot(ds, qs, preferred_element_type=F32), jnp.dot(pb, gs, preferred_element_type=F32)

    for s in range(2 * half // LEN):
        rows = slice(s * LEN, (s + 1) * LEN)
        at = s * LEN % half
        qref, qat, gref, gat = (queries, base, kept, own) if s * LEN < half else (came, qcol, came, gcol)
        key, value = kv[rows, :HD], kv[rows, HD:]
        value_t = value.T
        if (s + 1) * LEN < 2 * half:
            project(s + 1)
        early, late = slice(at, at + top), slice(at + top, at + LEN)
        dk0, dv0 = strip(key[:top], value[:top], value_t[:, :top], stacked(qref, early, qat), stacked(gref, early, gat))
        dk1, dv1 = strip(key, value, value_t, stacked(qref, late, qat), stacked(gref, late, gat))
        dk = jnp.concatenate([dk1[:top] + dk0, dk1[top:]], axis=0)
        dv = jnp.concatenate([dv1[:top] + dv0, dv1[top:]], axis=0)
        both = jnp.concatenate([(dk * scale).astype(BF), dv.astype(BF)], axis=1)
        dkvt[:, rows] = both.T

    for z in range(ZN):
        cols = pl.ds(level_at(z), 512)
        part = jnp.dot(dkvt[:, :half], sent[:, cols], preferred_element_type=F32)
        part += jnp.dot(dkvt[:, half:], came[:, cols], preferred_element_type=F32)
        block[...] = part.astype(BF).T
        for o2, target in enumerate((g0, g1, g2, g3)):
            for o1 in range(4):
                target[o1, z] = block[pl.ds(chunk_at(o1, o2), 32)]


def one_head(head, where, pieces, sent, came, queries, kept):
    tokens = 2 * queries.shape[0]
    vmem = pl.BlockSpec(memory_space=pltpu.VMEM)
    cols = 2 * HD
    return pl.pallas_call(
        head_kernel,
        in_specs=[pl.BlockSpec(memory_space=pltpu.SMEM)] * 2 + [vmem] * 8,
        out_specs=[vmem] * 4,
        out_shape=[jax.ShapeDtypeStruct((4, ZN, 32, cols), BF)] * 4,
        scratch_shapes=[
            pltpu.VMEM((D, cols), BF),
            pltpu.VMEM((tokens, cols), BF),
            pltpu.VMEM((cols, tokens), BF),
            pltpu.VMEM((512, cols), BF),
        ],
        compiler_params=pltpu.CompilerParams(vmem_limit_bytes=30 * 2**20),
        cost_estimate=pl.CostEstimate(flops=8_000_000_000, transcendentals=1_000_000, bytes_accessed=16_000_000),
        name="head",
    )(jnp.full((1,), head, jnp.int32), where, *pieces, sent, came, queries, kept)


def local(activations, queries, out_grad, lengths, norm_gain, key_master, value_master):
    r, z, x, y = (lax.axis_index(a) for a in ALL)
    first = r == 0
    where = jnp.stack([
        r,
        jnp.where(first, y, x), jnp.where(first, x, y),
        jnp.where(first, 1, 4), jnp.where(first, 4, 1),
        z, lengths[0], lengths[1],
    ]).astype(jnp.int32)

    own = cast(key_master, value_master)
    level = exchange(jnp.broadcast_to(own[None], (ZN, *own.shape)), "z")
    sent, kept = prepare(where, activations, queries, out_grad, norm_gain)
    came = to_partner(sent)
    gathered = [level]
    for o in (1, 2, 3):
        gathered.append(shift(level, 1, -o))
    pieces = []
    for head in range(2):
        block = jnp.stack([a[:, head] for a in gathered])
        pieces.append([block] + [shift(block, 2, -o) for o in (1, 2, 3)])
    parts = []
    for head in range(2):
        g = one_head(head, where, pieces[head], sent, came, queries, kept)
        got = [g[0]] + [shift(g[o], 2, o) for o in (1, 2, 3)]
        line = sum(a.astype(F32) for a in got).astype(BF)
        got = [line[0]] + [shift(line[o], 1, o) for o in (1, 2, 3)]
        parts.append(sum(a.astype(F32) for a in got).astype(BF))
    part = exchange(jnp.stack(parts, axis=1), "z")
    full = gather_sum(part)
    theirs = to_partner(full)
    square = squares(full, theirs)
    return finish(where, exchange(square, FSDP), full, theirs)


def solution(mesh):
    split = Mesh(mesh.devices.reshape(2, ZN, XN, YN), ALL)
    in_specs = (P(ALL, None), P(ALL, None), P(ALL, None), P(ALL), P(), P(FSDP, None), P(FSDP, None))
    out_specs = (P(FSDP, None), P(FSDP, None))


    return jax.shard_map(local, mesh=split, in_specs=in_specs, out_specs=out_specs, check_vma=False)
```

```python
import functools

import jax
import jax.numpy as jnp
from jax import lax
from jax.experimental import pallas as pl
from jax.experimental.pallas import tpu as pltpu
from jax.sharding import Mesh
from jax.sharding import PartitionSpec as P


D = 4096
HD = 128
GROUP = 4
LEN = 256
EPS = 1e-5
ZN, XN, YN = 8, 4, 4
FSDP = ("z", "x", "y")
ALL = ("r", "z", "x", "y")
BF = jnp.bfloat16
F32 = jnp.float32


def plane_pairs(phase, step):
    pairs = []
    for r in range(2):
        along_x = (r == 1) == (phase == 1)
        for z in range(ZN):
            for x in range(XN):
                for y in range(YN):
                    to = ((x + step) % XN, y) if along_x else (x, (y + step) % YN)
                    here = ((r * ZN + z) * XN + x) * YN + y
                    pairs.append((here, ((r * ZN + z) * XN + to[0]) * YN + to[1]))
    return pairs


def shift(a, phase, step):
    return lax.ppermute(a, ALL, plane_pairs(phase, step))


def to_partner(a):
    return lax.ppermute(a, "r", [(0, 1), (1, 0)])


def exchange(blocks, axes):
    return lax.all_to_all(blocks, axes, split_axis=0, concat_axis=0, tiled=True)


def in_hbm(a):
    return pltpu.with_memory_space_constraint(a, pltpu.HBM)


def cast_kernel(key, value, own, key_in, value_in, sems):
    cols = pl.ds(pl.multiple_of(lax.axis_index("r") * 2 * HD, 2 * HD), 2 * HD)
    loads = [
        pltpu.make_async_copy(key.at[:, cols], key_in, sems.at[0]),
        pltpu.make_async_copy(value.at[:, cols], value_in, sems.at[1]),
    ]
    for c in loads:
        c.start()
    for c in loads:
        c.wait()
    for h in range(2):
        own[h, :, :HD] = key_in[:, h * HD : (h + 1) * HD].astype(BF)
        own[h, :, HD:] = value_in[:, h * HD : (h + 1) * HD].astype(BF)


def cast(key, value):
    rows = key.shape[0]
    hbm = pl.BlockSpec(memory_space=pltpu.HBM)
    return pl.pallas_call(
        cast_kernel,
        in_specs=[hbm, hbm],
        out_specs=pl.BlockSpec(memory_space=pltpu.VMEM),
        out_shape=pltpu.VMEM((2, rows, 2 * HD), BF),
        scratch_shapes=[
            pltpu.VMEM((rows, 2 * HD), F32),
            pltpu.VMEM((rows, 2 * HD), F32),
            pltpu.SemaphoreType.DMA((2,)),
        ],
        compiler_params=pltpu.CompilerParams(vmem_limit_bytes=4 * 2**20),
        name="cast",
    )(in_hbm(key), in_hbm(value))


ROWS = 64


def prep_kernel(where, act, queries, grad, gain, send, kept, rows_in, grad_in, gain_in, sems):
    tokens, half = act.shape[0], queries.shape[1] // 2
    steps = tokens // ROWS
    mine = pl.multiple_of(where[0] * half, half)
    other = pl.multiple_of((1 - where[0]) * half, half)
    swap = pltpu.make_async_copy(queries.at[:, pl.ds(other, half)], send.at[:, pl.ds(D, half)], sems.at[2 * steps])

    def loads(i):
        at = pl.ds(pl.multiple_of(i * ROWS, ROWS), ROWS)
        return (
            pltpu.make_async_copy(act.at[at], rows_in.at[at], sems.at[i]),
            pltpu.make_async_copy(grad.at[at], grad_in.at[at], sems.at[steps + i]),
        )

    gain_load = pltpu.make_async_copy(gain, gain_in, sems.at[2 * steps + 1])
    gain_load.start()
    for i in range(steps):
        for c in loads(i):
            c.start()
    swap.start()
    gain_load.wait()
    zero = jnp.zeros((ROWS, half), BF)

    def step(i, _):
        at = pl.ds(pl.multiple_of(i * ROWS, ROWS), ROWS)
        for c in loads(i):
            c.wait()
        a = rows_in[at].astype(F32)
        inverse = lax.rsqrt(jnp.mean(a * a, axis=-1, keepdims=True) + EPS)
        send[at, :D] = (a * inverse * gain_in[...]).astype(BF)
        seq = i // (LEN // ROWS)
        live = i * ROWS - seq * LEN + lax.broadcasted_iota(jnp.int32, (ROWS, 1), 0) < where[6 + seq]
        send[at, D + half :] = jnp.where(live, grad_in[at, pl.ds(other, half)], zero)
        kept[at] = jnp.where(live, grad_in[at, pl.ds(mine, half)], zero)
        return 0

    lax.fori_loop(0, steps, step, 0)
    swap.wait()


def prepare(where, act, queries, grad, gain):
    tokens, width = act.shape[0], queries.shape[1]
    vmem = pl.BlockSpec(memory_space=pltpu.VMEM)
    smem = pl.BlockSpec(memory_space=pltpu.SMEM)
    hbm = pl.BlockSpec(memory_space=pltpu.HBM)
    return pl.pallas_call(
        prep_kernel,
        in_specs=[smem, hbm, hbm, hbm, hbm],
        out_specs=[vmem, vmem],
        out_shape=[
            pltpu.VMEM((tokens, D + width), BF),
            pltpu.VMEM((tokens, width // 2), BF),
        ],
        scratch_shapes=[
            pltpu.VMEM((tokens, D), BF),
            pltpu.VMEM((tokens, width), BF),
            pltpu.VMEM((1, D), F32),
            pltpu.SemaphoreType.DMA((2 * (tokens // ROWS) + 2,)),
        ],
        compiler_params=pltpu.CompilerParams(vmem_limit_bytes=24 * 2**20),
        cost_estimate=pl.CostEstimate(flops=1_000_000_000, transcendentals=512, bytes_accessed=16_000_000),
        name="prep",
    )(where, *(in_hbm(a) for a in (act, queries, grad, gain.reshape(1, D))))


def sum_kernel(parts, full):
    full[...] = functools.reduce(jnp.add, [parts[i].astype(F32) for i in range(ZN)])


def gather_sum(parts):
    vmem = pl.BlockSpec(memory_space=pltpu.VMEM)
    return pl.pallas_call(
        sum_kernel,
        in_specs=[vmem],
        out_specs=vmem,
        out_shape=pltpu.VMEM(parts.shape[1:], F32),
        compiler_params=pltpu.CompilerParams(vmem_limit_bytes=4 * 2**20),
        name="gather_sum",
    )(parts)


def square_kernel(full, theirs, square):
    total = jnp.sum(full[...] * full[...]) + jnp.sum(theirs[...] * theirs[...])
    square[...] = jnp.full(square.shape, total, F32)


def squares(full, theirs):
    vmem = pl.BlockSpec(memory_space=pltpu.VMEM)
    return pl.pallas_call(
        square_kernel,
        in_specs=[vmem] * 2,
        out_specs=vmem,
        out_shape=pltpu.VMEM((128, 1, 128), F32),
        compiler_params=pltpu.CompilerParams(vmem_limit_bytes=4 * 2**20),
        name="squares",
    )(full, theirs)


def finish_kernel(where, squares, full, theirs, key, value):
    total = jnp.sum(squares[...]) / 128
    scale = jnp.sqrt(jnp.float32(2 * D * 512)) / jnp.sqrt(total + 1e-6)
    for r in range(2):
        for h in range(2):
            both = jnp.where(where[0] == r, full[h], theirs[h]) * scale
            cols = slice((2 * r + h) * HD, (2 * r + h + 1) * HD)
            key[:, cols] = both[:, :HD]
            value[:, cols] = both[:, HD:]


def finish(where, squares, full, theirs):
    vmem = pl.BlockSpec(memory_space=pltpu.VMEM)
    like = jax.ShapeDtypeStruct((32, 4 * HD), F32)
    return pl.pallas_call(
        finish_kernel,
        in_specs=[pl.BlockSpec(memory_space=pltpu.SMEM)] + [vmem] * 3,
        out_specs=[vmem] * 2,
        out_shape=[like, like],
        compiler_params=pltpu.CompilerParams(vmem_limit_bytes=4 * 2**20),
        name="finish",
    )(where, squares, full, theirs)


NT = (((1,), (1,)), ((), ()))


def head_kernel(which, where, w0, w1, w2, w3, sent, came, queries, kept, g0, g1, g2, g3, w, kv, dkvt, block):
    half = queries.shape[0]
    wide = GROUP * HD
    own = pl.multiple_of(which[0] * wide, wide)
    base = pl.multiple_of(where[0] * (queries.shape[1] // 2) + own, wide)
    qcol = D + own
    gcol = D + queries.shape[1] // 2 + own
    p1, p2, s1, s2 = where[1], where[2], where[3], where[4]

    def chunk_at(o1, o2):
        return pl.multiple_of((lax.rem(p1 + o1, 4) * s1 + lax.rem(p2 + o2, 4) * s2) * 32, 32)

    def level_at(i):
        return i * 512

    for o2, source in enumerate((w0, w1, w2, w3)):
        for o1 in range(4):
            at = chunk_at(o1, o2)
            for z in range(ZN):
                w[pl.ds(level_at(z) + at, 32)] = source[o1, z]

    def project(s):
        source = sent if s * LEN < half else came
        at = s * LEN % half
        kv[s * LEN : (s + 1) * LEN] = jnp.dot(source[at : at + LEN, :D], w[...], preferred_element_type=F32).astype(BF)

    project(0)
    scale = 1.0 / HD**0.5
    top = HD
    below = lax.broadcasted_iota(jnp.int32, (top, top), 0) <= lax.broadcasted_iota(jnp.int32, (top, top), 1)

    def stacked(ref, rows, col):
        return jnp.concatenate([ref[rows, pl.ds(col + g * HD, HD)] for g in range(GROUP)], axis=0)

    def soft(parts):
        peak = functools.reduce(jnp.maximum, [jnp.max(a, axis=0, keepdims=True) for a in parts])
        parts = [jnp.exp(a - peak) for a in parts]
        inverse = 1.0 / functools.reduce(jnp.add, [jnp.sum(a, axis=0, keepdims=True) for a in parts])
        return [a * inverse for a in parts]

    def strip(key, value, value_t, qs, gs):
        keys = key.shape[0]
        score = lax.dot_general(key, qs, NT, preferred_element_type=F32)
        dp = lax.dot_general(value, gs, NT, preferred_element_type=F32)
        ps, pbs = [], []
        for g in range(GROUP):
            cols = slice(g * top, (g + 1) * top)
            parts = [score[i : i + top, cols] * scale for i in range(0, keys, top)]
            parts[-1] = jnp.where(below, parts[-1], -1e30)
            p = jnp.concatenate(soft(parts), axis=0)
            ps.append(p)
            pbs.append(p.astype(BF))
        pb = jnp.concatenate(pbs, axis=1)
        out_t = jnp.dot(value_t, pb, preferred_element_type=F32).astype(BF).astype(F32)
        delta = jnp.sum(gs.T.astype(F32) * out_t, axis=0, keepdims=True)
        ds = []
        for g in range(GROUP):
            cols = slice(g * top, (g + 1) * top)
            ds.append((ps[g] * (dp[:, cols] - delta[:, cols])).astype(BF))
        ds = jnp.concatenate(ds, axis=1)
        return jnp.dot(ds, qs, preferred_element_type=F32), jnp.dot(pb, gs, preferred_element_type=F32)

    for s in range(2 * half // LEN):
        rows = slice(s * LEN, (s + 1) * LEN)
        at = s * LEN % half
        qref, qat, gref, gat = (queries, base, kept, own) if s * LEN < half else (came, qcol, came, gcol)
        key, value = kv[rows, :HD], kv[rows, HD:]
        value_t = value.T
        if (s + 1) * LEN < 2 * half:
            project(s + 1)
        early, late = slice(at, at + top), slice(at + top, at + LEN)
        dk0, dv0 = strip(key[:top], value[:top], value_t[:, :top], stacked(qref, early, qat), stacked(gref, early, gat))
        dk1, dv1 = strip(key, value, value_t, stacked(qref, late, qat), stacked(gref, late, gat))
        dk = jnp.concatenate([dk1[:top] + dk0, dk1[top:]], axis=0)
        dv = jnp.concatenate([dv1[:top] + dv0, dv1[top:]], axis=0)
        both = jnp.concatenate([(dk * scale).astype(BF), dv.astype(BF)], axis=1)
        dkvt[:, rows] = both.T

    for z in range(ZN):
        cols = pl.ds(level_at(z), 512)
        part = jnp.dot(dkvt[:, :half], sent[:, cols], preferred_element_type=F32)
        part += jnp.dot(dkvt[:, half:], came[:, cols], preferred_element_type=F32)
        block[...] = part.astype(BF).T
        for o2, target in enumerate((g0, g1, g2, g3)):
            for o1 in range(4):
                target[o1, z] = block[pl.ds(chunk_at(o1, o2), 32)]


def one_head(head, where, pieces, sent, came, queries, kept):
    tokens = 2 * queries.shape[0]
    vmem = pl.BlockSpec(memory_space=pltpu.VMEM)
    cols = 2 * HD
    return pl.pallas_call(
        head_kernel,
        in_specs=[pl.BlockSpec(memory_space=pltpu.SMEM)] * 2 + [vmem] * 8,
        out_specs=[vmem] * 4,
        out_shape=[jax.ShapeDtypeStruct((4, ZN, 32, cols), BF)] * 4,
        scratch_shapes=[
            pltpu.VMEM((D, cols), BF),
            pltpu.VMEM((tokens, cols), BF),
            pltpu.VMEM((cols, tokens), BF),
            pltpu.VMEM((512, cols), BF),
        ],
        compiler_params=pltpu.CompilerParams(vmem_limit_bytes=30 * 2**20),
        cost_estimate=pl.CostEstimate(flops=8_000_000_000, transcendentals=1_000_000, bytes_accessed=16_000_000),
        name="head",
    )(jnp.full((1,), head, jnp.int32), where, *pieces, sent, came, queries, kept)


def local(activations, queries, out_grad, lengths, norm_gain, key_master, value_master):
    r, z, x, y = (lax.axis_index(a) for a in ALL)
    first = r == 0
    where = jnp.stack([
        r,
        jnp.where(first, y, x), jnp.where(first, x, y),
        jnp.where(first, 1, 4), jnp.where(first, 4, 1),
        z, lengths[0], lengths[1],
    ]).astype(jnp.int32)

    own = cast(key_master, value_master)
    level = exchange(jnp.broadcast_to(own[None], (ZN, *own.shape)), "z")
    sent, kept = prepare(where, activations, queries, out_grad, norm_gain)
    came = to_partner(sent)
    gathered = [level]
    for o in (1, 2, 3):
        gathered.append(shift(level, 1, -o))
    pieces = []
    for head in range(2):
        block = jnp.stack([a[:, head] for a in gathered])
        far = shift(block, 2, -2)
        pieces.append([block, shift(block, 2, -1), far, shift(block, 2, -3)])
    parts = []
    for head in range(2):
        g = one_head(head, where, pieces[head], sent, came, queries, kept)
        got = [g[0]] + [shift(g[o], 2, o) for o in (2, 1, 3)]
        line = sum(a.astype(F32) for a in got).astype(BF)
        got = [line[0]] + [shift(line[o], 1, o) for o in (1, 2, 3)]
        parts.append(sum(a.astype(F32) for a in got).astype(BF))
    part = exchange(jnp.stack(parts, axis=1), "z")
    full = gather_sum(part)
    theirs = to_partner(full)
    square = squares(full, theirs)
    return finish(where, exchange(square, FSDP), full, theirs)


def solution(mesh):
    split = Mesh(mesh.devices.reshape(2, ZN, XN, YN), ALL)
    in_specs = (P(ALL, None), P(ALL, None), P(ALL, None), P(ALL), P(), P(FSDP, None), P(FSDP, None))
    out_specs = (P(FSDP, None), P(FSDP, None))


    return jax.shard_map(local, mesh=split, in_specs=in_specs, out_specs=out_specs, check_vma=False)
```
